32 devices in a mesh: ta: 4 (over y, x), gz: 2 (over core), xy: 4 (over z).
Axes of the slice: x: 2, y: 2, z: 4, core: 2. Of those that a mesh axis runs over, the one named last changes fastest.
Arguments:
- source: float32 [2, 4, 3, 16, 16, 512], P(None, None, None, 'ta', 'gz', 'xy'), may hold values from -6 to 6
- iterate: float32 [2, 4, 3, 16, 16, 512], P(None, None, None, 'ta', 'gz', 'xy'), may hold values from -6 to 6
- gauge_links: float32 [4, 2, 3, 3, 16, 16, 512], P(None, None, None, None, 'ta', 'gz', 'xy'), may hold values from -2.4 to 2.4
- clover: float32 [2, 2, 6, 6, 16, 16, 512], P(None, None, None, None, 'ta', 'gz', 'xy'), may hold values from -0.6 to 0.6
- bc_sign: int32 [4], replicated, may hold values from -1 to 1, as said below
- null_store: bfloat16 [4, 4, 4, 2, 24, 12, 4, 4, 128], P('ta', 'gz', 'xy'), may hold values from -0.109375 to 0.109375
- block_slot: int32 [4, 4, 4], P('ta', 'gz', 'xy'), may hold values from 0 to 1, as said below
- coarse_links: float32 [9, 2, 24, 24, 4, 4, 4, 8], P(None, None, None, None, 'ta', 'gz', 'xy'), may hold values from -0.2 to 0.2
Outputs:
- new_iterate: float32 [2, 4, 3, 16, 16, 512], P(None, None, None, 'ta', 'gz', 'xy')
- new_residual: float32 [2, 4, 3, 16, 16, 512], P(None, None, None, 'ta', 'gz', 'xy')
The draws below stay inside these ranges and needn't reach their ends.
Inputs may be any that keep to these rules, and one draw needn't show every extreme that they name: `bc_sign`: each entry is -1 or +1. `block_slot`: within each device's block of 2 aggregate columns the entries are the numbers 0 to 1, each once.
All inputs are finite; a program needn't handle non-finite values.
Results may differ from the reference program's by a relative error of at most 0.0016.
Values sent between devices are 32-bit elements; how exact they have to be, the bound alone decides.
A program may use at most 256 MiB of HBM per device.

```python
import jax
import jax.numpy as jnp
import numpy as np
from jax import lax

NV = 24
BLK = 4
LT = 4
LZ = 8
LX = 4
LY = 32
CITERS = 4
NT = 16
NZ = 16
NXY = 512
CT = 4
CZ = 4
CX = 4
CY = 8


def draw_bc_sign(key, part):
    return 2 * jax.random.randint(key, (4,), 0, 2, dtype=jnp.int32) - 1


def draw_block_slot(key, part):
    dev_t = LT // BLK
    dev_z = LZ // BLK
    dev_x = LX // BLK
    count_t = CT // dev_t
    count_z = CZ // dev_z
    count_x = CX // dev_x
    per_device = dev_t * dev_z * dev_x
    scores = jax.random.randint(key, (count_t * count_z * count_x, per_device), 0, 1 << 16, dtype=jnp.int32)
    scores = scores * per_device + jnp.arange(per_device, dtype=jnp.int32)[None, :]
    ordering = jnp.argsort(scores, axis=1).astype(jnp.int32)
    ordering = ordering.reshape((count_t, count_z, count_x, dev_t, dev_z, dev_x))
    ordering = jnp.transpose(ordering, (0, 3, 1, 4, 2, 5))
    return ordering.reshape((CT, CZ, CX))


def level_of(own_key, shape, split, smallest, high):
    def one(dim, parts):
        draws = jax.random.uniform(jax.random.fold_in(jax.random.fold_in(own_key, 6), dim), (parts,), jnp.float32, smallest / len(split), high / len(split))
        return jnp.repeat(jnp.exp(draws), shape[dim] // parts).reshape((-1,) + (1,) * (len(shape) - dim - 1))

    loudness = one(*split[0])
    for cut in split[1:]:
        loudness = loudness * one(*cut)
    return loudness


def scatter_about(stream_key, shape, scale, bound, cuts=(), kind=jnp.bfloat16):
    values = scale * jax.random.normal(stream_key, shape, jnp.float32)
    if cuts:
        values = values * level_of(stream_key, shape, cuts, -0.22, 0.18)
    return jnp.clip(values, -bound, bound).astype(kind)


def setup_inputs(seed: int = 0) -> dict:
    key_list = jax.random.split(jax.random.key(seed), 9)
    source = scatter_about(key_list[0], (2, 4, 3, NT, NZ, NXY), 1.0, 6.0, ((3, 4), (4, 2), (5, 4)), jnp.float32)
    iterate = scatter_about(key_list[1], (2, 4, 3, NT, NZ, NXY), 1.0, 6.0, ((3, 4), (4, 2), (5, 4)), jnp.float32)
    gauge_links = scatter_about(key_list[2], (4, 2, 3, 3, NT, NZ, NXY), 0.4, 2.4, ((4, 4), (5, 2), (6, 4)), jnp.float32)
    clover = scatter_about(key_list[3], (2, 2, 6, 6, NT, NZ, NXY), 0.1, 0.6, ((4, 4), (5, 2), (6, 4)), jnp.float32)
    bc_sign = draw_bc_sign(jax.random.fold_in(key_list[8], 71), 0)
    null_store = scatter_about(key_list[5], (CT, CZ, CX, 2, NV, 12, BLK, BLK, BLK * LY), (12 * BLK ** 4) ** -0.5, 0.109375, ((0, 4), (1, 2), (2, 4)))
    block_slot = draw_block_slot(jax.random.fold_in(key_list[8], 71), 0)
    coarse_links = scatter_about(key_list[7], (9, 2, NV, NV, CT, CZ, CX, CY), 0.03, 0.2, ((4, 4), (5, 2), (6, 4)), jnp.float32)
    return {"source": source, "iterate": iterate, "gauge_links": gauge_links, "clover": clover, "bc_sign": bc_sign, "null_store": null_store, "block_slot": block_slot, "coarse_links": coarse_links}


MASS_TERM = 3.8
RELAX_WEIGHT = 0.4
HIGHEST = lax.Precision.HIGHEST


def chiral_blocks():
    identity = np.eye(2)
    nought = np.zeros((2, 2))
    flip_x = np.array([[0.0, 1.0], [1.0, 0.0]])
    flip_z = np.array([[1.0, 0.0], [0.0, -1.0]])
    rotate = np.array([[0.0, -1.0], [1.0, 0.0]])
    return [(identity, nought), (nought, -flip_z), (nought, -flip_x), (rotate, nought)]


def four_square(top_left, top_right, bottom_left, bottom_right):
    upper = np.concatenate([top_left, top_right], axis=1)
    lower = np.concatenate([bottom_left, bottom_right], axis=1)
    return np.concatenate([upper, lower], axis=0)


def spin_tables(direction, parity):
    upper_re, upper_im = chiral_blocks()[direction]
    identity = np.eye(2)
    nought = np.zeros((2, 2))
    gamma_re = four_square(nought, upper_re, upper_re.T, nought)
    gamma_im = four_square(nought, upper_im, -upper_im.T, nought)
    whole_re = np.eye(4) + parity * gamma_re
    whole_im = parity * gamma_im
    half_re = np.concatenate([identity, parity * upper_re], axis=1)
    half_im = np.concatenate([nought, parity * upper_im], axis=1)
    back_re = np.concatenate([identity, parity * upper_re.T], axis=0)
    back_im = np.concatenate([nought, -parity * upper_im.T], axis=0)
    return [np.asarray(matrix, np.float32) for matrix in (whole_re, whole_im, half_re, half_im, back_re, back_im)]


def spin_times(matrix_re, matrix_im, field):
    real_part = jnp.tensordot(matrix_re, field[0], axes=(1, 0), precision=HIGHEST) - jnp.tensordot(matrix_im, field[1], axes=(1, 0), precision=HIGHEST)
    imag_part = jnp.tensordot(matrix_re, field[1], axes=(1, 0), precision=HIGHEST) + jnp.tensordot(matrix_im, field[0], axes=(1, 0), precision=HIGHEST)
    return jnp.stack([real_part, imag_part])


def colour_times(link, field):
    real_part = 0.0
    imag_part = 0.0
    for column in range(3):
        link_re = link[0][:, column][None]
        link_im = link[1][:, column][None]
        field_re = field[0][:, column:column + 1]
        field_im = field[1][:, column:column + 1]
        real_part = real_part + link_re * field_re - link_im * field_im
        imag_part = imag_part + link_re * field_im + link_im * field_re
    return jnp.stack([real_part, imag_part])


def colour_dagger(link, field):
    real_part = 0.0
    imag_part = 0.0
    for column in range(3):
        link_re = link[0][column][None]
        link_im = link[1][column][None]
        field_re = field[0][:, column:column + 1]
        field_im = field[1][:, column:column + 1]
        real_part = real_part + link_re * field_re + link_im * field_im
        imag_part = imag_part + link_re * field_im - link_im * field_re
    return jnp.stack([real_part, imag_part])


def clover_times(clover, field):
    halves = []
    for chirality in range(2):
        chiral_part = field[:, 2 * chirality:2 * chirality + 2]
        chiral_part = chiral_part.reshape((2, 6) + chiral_part.shape[3:])
        matrix_re = clover[chirality, 0]
        matrix_im = clover[chirality, 1]
        real_part = 0.0
        imag_part = 0.0
        for column in range(6):
            real_part = real_part + matrix_re[:, column] * chiral_part[0, column][None] - matrix_im[:, column] * chiral_part[1, column][None]
            imag_part = imag_part + matrix_re[:, column] * chiral_part[1, column][None] + matrix_im[:, column] * chiral_part[0, column][None]
        halves.append(jnp.stack([real_part, imag_part]).reshape((2, 2, 3) + chiral_part.shape[2:]))
    return jnp.concatenate(halves, axis=1)


def along_y(field, forward):
    column_y = jnp.arange(field.shape[-1], dtype=jnp.int32) % LY
    if forward:
        return jnp.where(column_y == LY - 1, jnp.roll(field, LY - 1, axis=-1), jnp.roll(field, -1, axis=-1))
    return jnp.where(column_y == 0, jnp.roll(field, 1 - LY, axis=-1), jnp.roll(field, 1, axis=-1))


def neighbour(field, direction, forward):
    offset = -1 if forward else 1
    if direction == 0:
        return jnp.roll(field, offset, axis=-3)
    if direction == 1:
        return jnp.roll(field, offset, axis=-2)
    if direction == 2:
        return jnp.roll(field, offset * LY, axis=-1)
    return along_y(field, forward)


def edge_factors(bc_sign, shape):
    count_t, count_z, count_xy = shape
    flat_index = jnp.arange(count_xy, dtype=jnp.int32)
    places = [(jnp.arange(count_t, dtype=jnp.int32)[:, None, None], count_t),
              (jnp.arange(count_z, dtype=jnp.int32)[None, :, None], count_z),
              ((flat_index // LY)[None, None, :], count_xy // LY),
              ((flat_index % LY)[None, None, :], LY)]
    factors = []
    for direction in range(4):
        where_now, extent = places[direction]
        flipped = bc_sign[direction].astype(jnp.float32)
        factors.append((jnp.where(where_now == extent - 1, flipped, 1.0), jnp.where(where_now == 0, flipped, 1.0)))
    return factors


def fine_apply(field, gauge_links, clover, factors):
    result = MASS_TERM * field + clover_times(clover, field)
    for direction in range(4):
        minus_tables = spin_tables(direction, -1)
        plus_tables = spin_tables(direction, 1)
        ahead = colour_times(gauge_links[direction], neighbour(field, direction, True) * factors[direction][0])
        behind = colour_dagger(neighbour(gauge_links[direction], direction, False), neighbour(field, direction, False) * factors[direction][1])
        result = result - 0.5 * (spin_times(minus_tables[0], minus_tables[1], ahead) + spin_times(plus_tables[0], plus_tables[1], behind))
    return result


def source_index(block_slot):
    dev_t, dev_z, dev_x = LT // BLK, LZ // BLK, LX // BLK
    count_t, count_z, count_x = block_slot.shape
    base_t = jnp.arange(count_t, dtype=jnp.int32)[:, None, None] // dev_t * dev_t
    base_z = jnp.arange(count_z, dtype=jnp.int32)[None, :, None] // dev_z * dev_z
    base_x = jnp.arange(count_x, dtype=jnp.int32)[None, None, :] // dev_x * dev_x
    slot_t = block_slot // (dev_z * dev_x)
    slot_z = block_slot // dev_x % dev_z
    slot_x = block_slot % dev_x
    return (((base_t + slot_t) * count_z + base_z + slot_z) * count_x + base_x + slot_x).astype(jnp.int32)


def column_layout(field):
    width = BLK * LY
    shaped = field.reshape((2, 12, CT, BLK, CZ, BLK, CX, width))
    return jnp.moveaxis(shaped, 2, 0)


def restrict_all(rounded, null_store, indices):
    columns = column_layout(rounded)
    flat_store = null_store.reshape((-1,) + null_store.shape[3:])

    def one_slice(inputs):
        field_part, index_part = inputs
        null_rows = jnp.take(flat_store, index_part.reshape(-1), axis=0).astype(jnp.float32)
        null_rows = null_rows.reshape((CZ, CX) + null_rows.shape[1:])
        field_part = field_part.astype(jnp.float32)
        turned = jnp.stack([field_part[1], -field_part[0]])
        paired = jnp.stack([field_part, turned])
        return jnp.einsum('zxpvsabw,qpsazbxw->qvzxw', null_rows, paired, precision=HIGHEST)

    coarse = lax.map(one_slice, (columns, indices))
    coarse = coarse.reshape(coarse.shape[:5] + (BLK, CY, BLK)).sum(axis=(5, 7))
    return jnp.transpose(coarse, (1, 2, 0, 3, 4, 5))


def prolong_all(coarse_round, null_store, indices):
    width = BLK * LY
    per_slice = jnp.moveaxis(coarse_round, 2, 0)
    flat_store = null_store.reshape((-1,) + null_store.shape[3:])

    def one_slice(inputs):
        coarse_part, index_part = inputs
        null_rows = jnp.take(flat_store, index_part.reshape(-1), axis=0).astype(jnp.float32)
        null_rows = null_rows.reshape((CZ, CX) + null_rows.shape[1:])
        coarse_part = coarse_part.astype(jnp.float32)
        spread = jnp.broadcast_to(coarse_part[..., None, :, None], coarse_part.shape[:4] + (BLK, CY, BLK))
        spread = spread.reshape(coarse_part.shape[:4] + (width,))
        mixture = jnp.stack([jnp.stack([spread[0], -spread[1]]), jnp.stack([spread[1], spread[0]])])
        return jnp.einsum('zxpvsabw,qpvzxw->qsazbxw', null_rows, mixture, precision=HIGHEST)

    fine = lax.map(one_slice, (per_slice, indices))
    fine = jnp.moveaxis(fine, 0, 2)
    return fine.reshape((2, 4, 3, CT * BLK, CZ * BLK, CX * width))


def block_times(block_links, stacked):
    links_re = block_links[:, 0]
    links_im = block_links[:, 1]
    vector_re = stacked[:, 0]
    vector_im = stacked[:, 1]
    real_part = jnp.einsum('kijabcd,kjabcd->iabcd', links_re, vector_re, precision=HIGHEST) - jnp.einsum('kijabcd,kjabcd->iabcd', links_im, vector_im, precision=HIGHEST)
    imag_part = jnp.einsum('kijabcd,kjabcd->iabcd', links_re, vector_im, precision=HIGHEST) + jnp.einsum('kijabcd,kjabcd->iabcd', links_im, vector_re, precision=HIGHEST)
    return jnp.stack([real_part, imag_part])


def coarse_apply(vector, coarse_links):
    neighbours = [vector,
                  jnp.roll(vector, -1, 2), jnp.roll(vector, 1, 2),
                  jnp.roll(vector, -1, 3), jnp.roll(vector, 1, 3),
                  jnp.roll(vector, -1, 4), jnp.roll(vector, 1, 4),
                  jnp.roll(vector, -1, 5), jnp.roll(vector, 1, 5)]
    return 2.0 * vector + block_times(coarse_links, jnp.stack(neighbours))


def reference(source, iterate, gauge_links, clover, bc_sign, null_store, block_slot, coarse_links):
    factors = edge_factors(bc_sign, source.shape[3:])
    residual_start = source - fine_apply(iterate, gauge_links, clover, factors)
    indices = source_index(block_slot)
    coarse_rhs = restrict_all(residual_start.astype(jnp.bfloat16), null_store, indices)
    coarse_sol = RELAX_WEIGHT * coarse_rhs
    for iteration in range(CITERS - 1):
        coarse_sol = coarse_sol + RELAX_WEIGHT * (coarse_rhs - coarse_apply(coarse_sol, coarse_links))
    correction = prolong_all(coarse_sol.astype(jnp.bfloat16), null_store, indices)
    new_iterate = iterate + correction
    new_residual = residual_start - fine_apply(correction, gauge_links, clover, factors)
    return new_iterate, new_residual
```

```python
import functools

import jax
import jax.numpy as jnp
from jax import lax
from jax.experimental import pallas as pl
from jax.experimental.pallas import tpu as pltpu
from jax.sharding import PartitionSpec as P

BLK = 4
LY = 32
CITERS = 4
MASS_TERM = 3.8
RELAX_WEIGHT = 0.4
HIGHEST = lax.Precision.HIGHEST
MESH = pl.DeviceIdType.MESH
F32 = jnp.float32

UPPER = [((0, 0), (1, 0)), ((0, 3), (1, 1)), ((1, 3), (0, 3)), ((1, 2), (0, 0))]
LOWER = [((0, 0), (1, 0)), ((0, 1), (1, 3)), ((1, 1), (0, 1)), ((1, 0), (0, 2))]


def add_turned(a, b, power):
    power %= 4
    if power == 0:
        return (a[0] + b[0], a[1] + b[1])
    if power == 1:
        return (a[0] - b[1], a[1] + b[0])
    if power == 2:
        return (a[0] - b[0], a[1] - b[1])
    return (a[0] + b[1], a[1] - b[0])


def project(psi, mu, forward):
    turn = 2 if forward else 0
    return [
        [add_turned(psi[row][c], psi[2 + UPPER[mu][row][0]][c], UPPER[mu][row][1] + turn) for c in range(3)]
        for row in range(2)
    ]


def rebuild(total, half, mu, forward):
    turn = 2 if forward else 0
    for row in range(2):
        index, power = LOWER[mu][row]
        for c in range(3):
            total[row][c] = add_turned(total[row][c], half[row][c], 0)
            total[2 + row][c] = add_turned(total[2 + row][c], half[index][c], power + turn)


def link_times(gauge, mu, t, half):
    out = [[None] * 3 for _ in range(2)]
    for a in range(3):
        for b in range(3):
            ur = gauge[mu, 0, a * 3 + b, t]
            ui = gauge[mu, 1, a * 3 + b, t]
            for s in range(2):
                hr, hi = half[s][b]
                term = (ur * hr - ui * hi, ur * hi + ui * hr)
                out[s][a] = term if b == 0 else add_turned(out[s][a], term, 0)
    return out


def link_dagger(gauge, mu, t, half):
    out = [[None] * 3 for _ in range(2)]
    for a in range(3):
        for b in range(3):
            ur = gauge[mu, 0, b * 3 + a, t]
            ui = gauge[mu, 1, b * 3 + a, t]
            for s in range(2):
                hr, hi = half[s][b]
                term = (ur * hr + ui * hi, ur * hi - ui * hr)
                out[s][a] = term if b == 0 else add_turned(out[s][a], term, 0)
    return out


def load_spinor(ref, t):
    return [[(ref[s * 3 + c, t], ref[12 + s * 3 + c, t]) for c in range(3)] for s in range(4)]


def load_half(ref, *lead):
    return [[(ref[(*lead, s * 3 + c)], ref[(*lead, 6 + s * 3 + c)]) for c in range(3)] for s in range(2)]


def store_half(ref, half, *lead):
    for s in range(2):
        for c in range(3):
            ref[(*lead, s * 3 + c)] = half[s][c][0]
            ref[(*lead, 6 + s * 3 + c)] = half[s][c][1]


def map_half(half, change):
    return [[(change(z[0]), change(z[1])) for z in row] for row in half]


def roll(value, shift, axis):
    shift %= value.shape[axis]
    return value if shift == 0 else pltpu.roll(value, shift, axis)


def split_columns(a, b, top):
    return (
        jnp.where(top, a, pltpu.roll(b, BLK, 0)),
        jnp.where(top, pltpu.roll(a, BLK, 0), b),
    )


def kernel(
    counts, bc_ref, slot_ref, src_hbm, it_hbm, ga_hbm, cl_hbm, nu_hbm, co_hbm, out_it, out_res,
    src, itv, ga, cl, nu, co, res, corr, nit, ht, gt, hb, ps, pr, rc, mrows, wbuf, rhs, wr, wz, part, wexp,
    load_sem, send_sem, recv_sem,
):
    T = itv.shape[1]
    loads = []
    for i, (a, b) in enumerate(
        [(it_hbm, itv), (ga_hbm, ga), (src_hbm, src), (cl_hbm, cl), (nu_hbm, nu), (co_hbm, co)]
    ):
        copy = pltpu.make_async_copy(a, b, load_sem.at[i])
        copy.start()
        loads.append(copy)

    names = ("ta", "gz", "xy")
    place = {n: lax.axis_index(n) for n in names}
    ahead = {n: {n: lax.rem(place[n] + 1, counts[n])} for n in names}
    behind = {n: {n: lax.rem(place[n] + counts[n] - 1, counts[n])} for n in names}
    barrier = pltpu.get_barrier_semaphore()
    for n in names:
        for target in (ahead[n], behind[n]):
            pl.semaphore_signal(barrier, inc=1, device_id=target, device_id_type=MESH)
    pl.semaphore_wait(barrier, 6)

    def send(number, source, target, device):
        copy = pltpu.make_async_remote_copy(
            src_ref=source, dst_ref=target, send_sem=send_sem.at[number], recv_sem=recv_sem.at[number],
            device_id=device, device_id_type=MESH,
        )
        copy.start()
        return copy

    row = lax.broadcasted_iota(jnp.int32, (8, 128), 0)
    lane = lax.broadcasted_iota(jnp.int32, (8, 128), 1)
    column_y = lane & (LY - 1)
    sign = [bc_ref[mu].astype(F32) for mu in range(4)]
    last = [jnp.where(place[n] == counts[n] - 1, sign[i], 1.0) for i, n in enumerate(names)]
    first = [jnp.where(place[n] == 0, sign[i], 1.0) for i, n in enumerate(names)]

    def subtract_fine(d, field, base, out, before_local):
        def prepare(t, carry):
            psi = load_spinor(field, t)
            store_half(ht, project(psi, 0, True), d, t)
            store_half(gt, link_dagger(ga, 0, t, project(psi, 0, False)), d, t + 1)
            for mu in (1, 2):
                store_half(hb, project(psi, mu, True), 2 * mu - 2, t)
                store_half(hb, link_dagger(ga, mu, t, project(psi, mu, False)), 2 * mu - 1, t)
            return carry

        lax.fori_loop(0, T, prepare, 0)

        def pack(c, carry):
            z0, z1, x0, x1 = hb[0, 0, c], roll(hb[1, 0, c], 1, 0), hb[2, 0, c], roll(hb[3, 0, c], LY, 1)
            for t in range(1, T):
                z0 = jnp.where(row == t, roll(hb[0, t, c], t, 0), z0)
                z1 = jnp.where(row == t, roll(hb[1, t, c], t + 1, 0), z1)
                mine = (lane // LY) == t
                x0 = jnp.where(mine, roll(hb[2, t, c], LY * t, 1), x0)
                x1 = jnp.where(mine, roll(hb[3, t, c], LY * t + LY, 1), x1)
            ps[d, 0, c] = z0
            ps[d, 1, c] = z1
            ps[d, 2, c] = x0
            ps[d, 3, c] = x1
            return carry

        base_number = d * 6
        copies = [
            send(base_number, ht.at[d, 0], ht.at[d, T], behind["ta"]),
            send(base_number + 1, gt.at[d, T], gt.at[d, 0], ahead["ta"]),
        ]
        lax.fori_loop(0, 12, pack, 0)
        for kind, target in enumerate((behind["gz"], ahead["gz"], behind["xy"], ahead["xy"])):
            copies.append(send(base_number + 2 + kind, ps.at[d, kind], pr.at[d, kind], target))

        before_local()

        def local(t, carry):
            psi = load_spinor(field, t)
            total = [[(jnp.zeros((8, 128), F32), jnp.zeros((8, 128), F32)) for _ in range(3)] for _ in range(4)]

            def up(v):
                return jnp.where(column_y == LY - 1, roll(v, LY - 1, 1) * sign[3], roll(v, -1, 1))

            def down(v):
                return jnp.where(column_y == 0, roll(v, 1 - LY, 1) * sign[3], roll(v, 1, 1))

            rebuild(total, link_times(ga, 3, t, map_half(project(psi, 3, True), up)), 3, True)
            rebuild(total, map_half(link_dagger(ga, 3, t, project(psi, 3, False)), down), 3, False)
            for ch in range(2):
                for i in range(6):
                    s, c = 2 * ch + i // 3, i % 3
                    re, im = psi[s][c][0] * MASS_TERM, psi[s][c][1] * MASS_TERM
                    for j in range(6):
                        vr, vi = psi[2 * ch + j // 3][j % 3]
                        mr, mi = cl[ch, 0, i * 6 + j, t], cl[ch, 1, i * 6 + j, t]
                        re = re + (mr * vr - mi * vi)
                        im = im + (mr * vi + mi * vr)
                    k = s * 3 + c
                    out[k, t] = base[k, t] - re + 0.5 * total[s][c][0]
                    out[12 + k, t] = base[12 + k, t] - im + 0.5 * total[s][c][1]
            return carry

        lax.fori_loop(0, T, local, 0)
        for copy in copies:
            copy.wait()

        def unpack(c, carry):
            z0, z1 = pr[d, 0, c] * last[1], pr[d, 1, c] * first[1]
            x0, x1 = pr[d, 2, c] * last[2], pr[d, 3, c] * first[2]
            for t in range(T):
                hb[0, t, c] = jnp.where(row == 7, roll(z0, 7 - t, 0), roll(hb[0, t, c], -1, 0))
                hb[1, t, c] = jnp.where(row == 0, roll(z1, -t, 0), roll(hb[1, t, c], 1, 0))
                hb[2, t, c] = jnp.where(lane >= 128 - LY, roll(x0, 128 - LY - LY * t, 1), roll(hb[2, t, c], -LY, 1))
                hb[3, t, c] = jnp.where(lane < LY, roll(x1, -LY * t, 1), roll(hb[3, t, c], LY, 1))
            return carry

        lax.fori_loop(0, 12, unpack, 0)

        def finish(t, carry):
            total = [[(jnp.zeros((8, 128), F32), jnp.zeros((8, 128), F32)) for _ in range(3)] for _ in range(4)]
            edge = jnp.where(t == T - 1, last[0], 1.0)
            rebuild(total, link_times(ga, 0, t, map_half(load_half(ht, d, t + 1), lambda v: v * edge)), 0, True)
            low = jnp.where(t == 0, first[0], 1.0)
            rebuild(total, map_half(load_half(gt, d, t), lambda v: v * low), 0, False)
            for mu in (1, 2):
                rebuild(total, link_times(ga, mu, t, load_half(hb, 2 * mu - 2, t)), mu, True)
                rebuild(total, load_half(hb, 2 * mu - 1, t), mu, False)
            for s in range(4):
                for c in range(3):
                    k = s * 3 + c
                    out[k, t] = out[k, t] + 0.5 * total[s][c][0]
                    out[12 + k, t] = out[12 + k, t] + 0.5 * total[s][c][1]
            return carry

        lax.fori_loop(0, T, finish, 0)

    mrows[...] = jnp.zeros(mrows.shape, F32)
    loads[0].wait()
    loads[1].wait()

    def rest():
        loads[2].wait()
        loads[3].wait()

    subtract_fine(0, itv, src, res, rest)

    top = row < BLK

    def to_columns(k, carry):
        for pair in range(2):
            parts = split_columns(res[k, 2 * pair], res[k, 2 * pair + 1], top)
            for col in range(2):
                rc[col, k, pl.ds(8 * pair, 8), :] = parts[col].astype(jnp.bfloat16).astype(F32)
        return carry

    lax.fori_loop(0, 24, to_columns, 0)
    loads[4].wait()
    group = 4
    for col in range(2):
        slot = slot_ref[col]

        def restrict(g, carry):
            re = [jnp.zeros((16, 128), F32) for _ in range(group)]
            im = [jnp.zeros((16, 128), F32) for _ in range(group)]
            for s in range(12):
                fr, fi = rc[col, s], rc[col, 12 + s]
                for j in range(group):
                    nr = nu[slot, 0, g * group + j, s].astype(F32)
                    ni = nu[slot, 1, g * group + j, s].astype(F32)
                    re[j] = re[j] + (nr * fr + ni * fi)
                    im[j] = im[j] + (nr * fi - ni * fr)
            for j in range(group):
                mrows[col, 0, pl.ds(g * group + j, 1), :] = jnp.sum(re[j], axis=0, keepdims=True)
                mrows[col, 1, pl.ds(g * group + j, 1), :] = jnp.sum(im[j], axis=0, keepdims=True)
            return carry

        lax.fori_loop(0, 24 // group, restrict, 0)
    chooser = ((column_y // BLK) == row).astype(F32)
    for col in range(2):
        for ri in range(2):
            value = lax.dot_general(
                chooser, mrows[col, ri], (((1,), (1,)), ((), ())), precision=HIGHEST, preferred_element_type=F32
            )
            rhs[col, ri] = value
            wbuf[0, col, ri] = RELAX_WEIGHT * value
    loads[5].wait()

    nv = co.shape[-1]
    block = 8
    for it in range(CITERS - 1):
        number = 12 + it * 6
        copies = [
            send(number, wbuf.at[it], wr.at[it, 0], behind["ta"]),
            send(number + 1, wbuf.at[it], wr.at[it, 1], ahead["ta"]),
            send(number + 2, wbuf.at[it], wr.at[it, 2], behind["xy"]),
            send(number + 3, wbuf.at[it], wr.at[it, 3], ahead["xy"]),
            send(number + 4, wbuf.at[it, 0], wz.at[it, 0], behind["gz"]),
            send(number + 5, wbuf.at[it, 1], wz.at[it, 1], ahead["gz"]),
        ]

        def products(col, pairs, i, re, im):
            for k, vr, vi in pairs:
                yr, yi = co[k, 0, i, col], co[k, 1, i, col]
                a, b = yr * vr - yi * vi, yr * vi + yi * vr
                re, im = (a, b) if re is None else (re + a, im + b)
            return re, im

        for col in range(2):
            own = [wbuf[it, col, ri] for ri in range(2)]
            other = [wbuf[it, 1 - col, ri, :, :nv] for ri in range(2)]
            pairs = [
                (0, own[0][:, :nv], own[1][:, :nv]),
                (3 if col == 0 else 4, other[0], other[1]),
                (7, roll(own[0], -1, 0)[:, :nv], roll(own[1], -1, 0)[:, :nv]),
                (8, roll(own[0], 1, 0)[:, :nv], roll(own[1], 1, 0)[:, :nv]),
            ]

            def near(g, carry):
                for j in range(block):
                    i = g * block + j
                    re, im = products(col, pairs, i, None, None)
                    part[col, 0, i] = re
                    part[col, 1, i] = im
                return carry

            lax.fori_loop(0, nv // block, near, 0)
        for copy in copies:
            copy.wait()
        for col in range(2):
            pairs = [
                (k, wr[it, d, col, 0, :, :nv], wr[it, d, col, 1, :, :nv])
                for k, d in ((1, 0), (2, 1), (5, 2), (6, 3))
            ]
            far_z = 1 - col
            pairs.append((4 if col == 0 else 3, wz[it, far_z, 0, :, :nv], wz[it, far_z, 1, :, :nv]))

            def far(g, carry):
                new_re, new_im = carry
                for j in range(block):
                    i = g * block + j
                    re, im = products(col, pairs, i, part[col, 0, i], part[col, 1, i])
                    new_re = jnp.where(lane == i, jnp.sum(re, axis=1, keepdims=True), new_re)
                    new_im = jnp.where(lane == i, jnp.sum(im, axis=1, keepdims=True), new_im)
                return new_re, new_im

            zero = jnp.zeros((8, 128), F32)
            applied = lax.fori_loop(0, nv // block, far, (zero, zero))
            for ri in range(2):
                w = wbuf[it, col, ri]
                wbuf[it + 1, col, ri] = w + RELAX_WEIGHT * (rhs[col, ri] - (2.0 * w + applied[ri]))

    for col in range(2):
        for ri in range(2):
            w = wbuf[CITERS - 1, col, ri].astype(jnp.bfloat16).astype(F32)
            wexp[col, ri] = lax.dot_general(
                w, chooser, (((0,), (0,)), ((), ())), precision=HIGHEST, preferred_element_type=F32
            )
    spins = 3
    step = 4
    for col in range(2):
        slot = slot_ref[col]

        def some_spins(q, carry):
            def over(g, totals):
                totals = list(totals)
                for j in range(step):
                    c = g * step + j
                    vr = wexp[col, 0, pl.ds(c, 1), :]
                    vi = wexp[col, 1, pl.ds(c, 1), :]
                    for m in range(spins):
                        nr = nu[slot, 0, c, q * spins + m].astype(F32)
                        ni = nu[slot, 1, c, q * spins + m].astype(F32)
                        totals[2 * m] = totals[2 * m] + (nr * vr - ni * vi)
                        totals[2 * m + 1] = totals[2 * m + 1] + (nr * vi + ni * vr)
                return tuple(totals)

            zero = jnp.zeros((16, 128), F32)
            totals = lax.fori_loop(0, nv // step, over, (zero,) * (2 * spins))
            for m in range(spins):
                rc[col, q * spins + m] = totals[2 * m]
                rc[col, 12 + q * spins + m] = totals[2 * m + 1]
            return carry

        lax.fori_loop(0, 12 // spins, some_spins, 0)

    def from_columns(k, carry):
        for pair in range(2):
            part_0 = rc[0, k, pl.ds(8 * pair, 8), :]
            part_1 = rc[1, k, pl.ds(8 * pair, 8), :]
            values = split_columns(part_0, part_1, top)
            for h in range(2):
                t = 2 * pair + h
                corr[k, t] = values[h]
                nit[k, t] = itv[k, t] + values[h]
        return carry

    lax.fori_loop(0, 24, from_columns, 0)
    store_it = pltpu.make_async_copy(nit, out_it, load_sem.at[6])
    store_it.start()
    subtract_fine(1, corr, res, res, lambda: None)
    store_res = pltpu.make_async_copy(res, out_res, load_sem.at[7])
    store_res.start()
    store_it.wait()
    store_res.wait()


def per_device(counts, source, iterate, gauge_links, clover, bc_sign, null_store, block_slot, coarse_links):
    lattice = source.shape[3:]
    T = lattice[0]
    spinor = (24,) + lattice
    columns = block_slot.size
    nv = null_store.shape[4]
    assert lattice == (BLK, 2 * BLK, BLK * LY) and columns == 2
    nulls = (columns,) + null_store.shape[3:6] + (BLK * BLK, BLK * LY)
    links = jnp.transpose(coarse_links, (0, 1, 2, 4, 5, 6, 7, 3))
    links = links.reshape(links.shape[:3] + (columns,) + links.shape[6:])
    gauge_shape = (4, 2, 9) + lattice
    clover_shape = (2, 2, 36) + lattice
    half = (12,) + lattice[1:]
    tile = lattice[1:]
    smem = pl.BlockSpec(memory_space=pltpu.SMEM)
    hbm = pl.BlockSpec(memory_space=pl.ANY)
    fine = jax.ShapeDtypeStruct(spinor, F32)
    n_copies = 12 + 6 * (CITERS - 1)
    outs = pl.pallas_call(
        functools.partial(kernel, counts),
        out_shape=(fine, fine),
        in_specs=[smem, smem] + [hbm] * 6,
        out_specs=(hbm, hbm),
        scratch_shapes=[
            pltpu.VMEM(spinor, F32),
            pltpu.VMEM(spinor, F32),
            pltpu.VMEM(gauge_shape, F32),
            pltpu.VMEM(clover_shape, F32),
            pltpu.VMEM(nulls, jnp.bfloat16),
            pltpu.VMEM(links.shape, F32),
            pltpu.VMEM(spinor, F32),
            pltpu.VMEM(spinor, F32),
            pltpu.VMEM(spinor, F32),
            pltpu.VMEM((2, T + 1) + half, F32),
            pltpu.VMEM((2, T + 1) + half, F32),
            pltpu.VMEM((4, T) + half, F32),
            pltpu.VMEM((2, 4) + half, F32),
            pltpu.VMEM((2, 4) + half, F32),
            pltpu.VMEM((columns, 24, BLK * BLK, BLK * LY), F32),
            pltpu.VMEM((columns, 2, 128, 128), F32),
            pltpu.VMEM((CITERS, columns, 2) + tile, F32),
            pltpu.VMEM((columns, 2) + tile, F32),
            pltpu.VMEM((CITERS - 1, 4, columns, 2) + tile, F32),
            pltpu.VMEM((CITERS - 1, 2, 2) + tile, F32),
            pltpu.VMEM((columns, 2, nv, 8, nv), F32),
            pltpu.VMEM((columns, 2, 128, 128), F32),
            pltpu.SemaphoreType.DMA((8,)),
            pltpu.SemaphoreType.DMA((n_copies,)),
            pltpu.SemaphoreType.DMA((n_copies,)),
        ],
        compiler_params=pltpu.CompilerParams(
            collective_id=0, has_side_effects=True, vmem_limit_bytes=67_043_328
        ),
    )(
        bc_sign,
        block_slot.reshape(-1),
        source.reshape(spinor),
        iterate.reshape(spinor),
        gauge_links.reshape(gauge_shape),
        clover.reshape(clover_shape),
        null_store.reshape(nulls),
        links,
    )
    return tuple(out.reshape(source.shape) for out in outs)


def solution(mesh):
    placed = (
        P(None, None, None, "ta", "gz", "xy"),
        P(None, None, None, "ta", "gz", "xy"),
        P(None, None, None, None, "ta", "gz", "xy"),
        P(None, None, None, None, "ta", "gz", "xy"),
        P(),
        P("ta", "gz", "xy", None, None, None, None, None, None),
        P("ta", "gz", "xy"),
        P(None, None, None, None, "ta", "gz", "xy", None),
    )
    return jax.shard_map(
        functools.partial(per_device, dict(mesh.shape)),
        mesh=mesh,
        in_specs=placed,
        out_specs=(P(None, None, None, "ta", "gz", "xy"), P(None, None, None, "ta", "gz", "xy")),
        check_vma=False,
    )
```

```python
import functools

import jax
import jax.numpy as jnp
from jax import lax
from jax.experimental import pallas as pl
from jax.experimental.pallas import tpu as pltpu
from jax.sharding import PartitionSpec as P

BLK = 4
LY = 32
CITERS = 4
MASS_TERM = 3.8
RELAX_WEIGHT = 0.4
HIGHEST = lax.Precision.HIGHEST
MESH = pl.DeviceIdType.MESH
LANES = 32
F32 = jnp.float32

UPPER = [((0, 0), (1, 0)), ((0, 3), (1, 1)), ((1, 3), (0, 3)), ((1, 2), (0, 0))]
LOWER = [((0, 0), (1, 0)), ((0, 1), (1, 3)), ((1, 1), (0, 1)), ((1, 0), (0, 2))]


def add_turned(a, b, power):
    power %= 4
    if power == 0:
        return (a[0] + b[0], a[1] + b[1])
    if power == 1:
        return (a[0] - b[1], a[1] + b[0])
    if power == 2:
        return (a[0] - b[0], a[1] - b[1])
    return (a[0] + b[1], a[1] - b[0])


def project(psi, mu, forward):
    turn = 2 if forward else 0
    return [
        [add_turned(psi[row][c], psi[2 + UPPER[mu][row][0]][c], UPPER[mu][row][1] + turn) for c in range(3)]
        for row in range(2)
    ]


def rebuild(total, half, mu, forward):
    turn = 2 if forward else 0
    for row in range(2):
        index, power = LOWER[mu][row]
        for c in range(3):
            total[row][c] = add_turned(total[row][c], half[row][c], 0)
            total[2 + row][c] = add_turned(total[2 + row][c], half[index][c], power + turn)


def link_times(gauge, mu, t, half):
    out = [[None] * 3 for _ in range(2)]
    for a in range(3):
        for b in range(3):
            ur = gauge[mu, 0, a * 3 + b, t]
            ui = gauge[mu, 1, a * 3 + b, t]
            for s in range(2):
                hr, hi = half[s][b]
                term = (ur * hr - ui * hi, ur * hi + ui * hr)
                out[s][a] = term if b == 0 else add_turned(out[s][a], term, 0)
    return out


def link_dagger(gauge, mu, t, half):
    out = [[None] * 3 for _ in range(2)]
    for a in range(3):
        for b in range(3):
            ur = gauge[mu, 0, b * 3 + a, t]
            ui = gauge[mu, 1, b * 3 + a, t]
            for s in range(2):
                hr, hi = half[s][b]
                term = (ur * hr + ui * hi, ur * hi - ui * hr)
                out[s][a] = term if b == 0 else add_turned(out[s][a], term, 0)
    return out


def load_spinor(ref, t):
    return [[(ref[s * 3 + c, t], ref[12 + s * 3 + c, t]) for c in range(3)] for s in range(4)]


def load_half(ref, *lead):
    return [[(ref[(*lead, s * 3 + c)], ref[(*lead, 6 + s * 3 + c)]) for c in range(3)] for s in range(2)]


def store_half(ref, half, *lead):
    for s in range(2):
        for c in range(3):
            ref[(*lead, s * 3 + c)] = half[s][c][0]
            ref[(*lead, 6 + s * 3 + c)] = half[s][c][1]


def map_half(half, change):
    return [[(change(z[0]), change(z[1])) for z in row] for row in half]


def roll(value, shift, axis):
    shift %= value.shape[axis]
    return value if shift == 0 else pltpu.roll(value, shift, axis)


def split_columns(a, b, top):
    return (
        jnp.where(top, a, pltpu.roll(b, BLK, 0)),
        jnp.where(top, pltpu.roll(a, BLK, 0), b),
    )


def kernel(
    counts, bc_ref, slot_ref, src_hbm, it_hbm, ga_hbm, cl_hbm, nu_hbm, co_hbm, out_it, out_res,
    src, itv, ga, cl, nu, co, res, corr, nit, ht, gt, hb, hs, ps, pr, rc, mrows, wbuf, rhs, wr, part, wexp,
    load_sem, send_sem, recv_sem,
):
    T = itv.shape[1]
    loads = []
    for i, (a, b) in enumerate(
        [(it_hbm, itv), (ga_hbm, ga), (src_hbm, src), (cl_hbm, cl), (nu_hbm, nu), (co_hbm, co)]
    ):
        copy = pltpu.make_async_copy(a, b, load_sem.at[i])
        copy.start()
        loads.append(copy)

    names = ("ta", "gz", "xy")
    place = {n: lax.axis_index(n) for n in names}
    ahead = {n: {n: lax.rem(place[n] + 1, counts[n])} for n in names}
    behind = {n: {n: lax.rem(place[n] + counts[n] - 1, counts[n])} for n in names}
    barrier = pltpu.get_barrier_semaphore()
    for n in names:
        for target in (ahead[n], behind[n]):
            pl.semaphore_signal(barrier, inc=1, device_id=target, device_id_type=MESH)

    def send(number, source, target, device):
        copy = pltpu.make_async_remote_copy(
            src_ref=source, dst_ref=target, send_sem=send_sem.at[number], recv_sem=recv_sem.at[number],
            device_id=device, device_id_type=MESH,
        )
        copy.start()
        return copy

    row = lax.broadcasted_iota(jnp.int32, (8, 128), 0)
    lane = lax.broadcasted_iota(jnp.int32, (8, 128), 1)
    column_y = lane & (LY - 1)
    sign = [bc_ref[mu].astype(F32) for mu in range(4)]
    last = [jnp.where(place[n] == counts[n] - 1, sign[i], 1.0) for i, n in enumerate(names)]
    first = [jnp.where(place[n] == 0, sign[i], 1.0) for i, n in enumerate(names)]

    def subtract_fine(d, field, base, out, before_local):
        def prepare(t, carry):
            psi = load_spinor(field, t)
            store_half(ht, project(psi, 0, True), d, t)
            store_half(gt, link_dagger(ga, 0, t, project(psi, 0, False)), d, t + 1)
            for mu in (1, 2):
                store_half(hb, project(psi, mu, True), 2 * mu - 2, t)
                store_half(hb, link_dagger(ga, mu, t, project(psi, mu, False)), 2 * mu - 1, t)
            return carry

        lax.fori_loop(0, T, prepare, 0)

        def pack(g, carry):
            for k in range(4):
                c = g * 4 + k
                z0, z1, x0, x1 = hb[0, 0, c], roll(hb[1, 0, c], 1, 0), hb[2, 0, c], roll(hb[3, 0, c], LY, 1)
                for t in range(1, T):
                    z0 = jnp.where(row == t, roll(hb[0, t, c], t, 0), z0)
                    z1 = jnp.where(row == t, roll(hb[1, t, c], t + 1, 0), z1)
                    mine = (lane // LY) == t
                    x0 = jnp.where(mine, roll(hb[2, t, c], LY * t, 1), x0)
                    x1 = jnp.where(mine, roll(hb[3, t, c], LY * t + LY, 1), x1)
                for kind, value in enumerate((z0, z1, x0, x1)):
                    ps[d, kind, c] = value
            return carry

        if d == 0:
            pl.semaphore_wait(barrier, 6)
        base_number = d * 6
        copies = [
            send(base_number, ht.at[d, 0], ht.at[d, T], behind["ta"]),
            send(base_number + 1, gt.at[d, T], gt.at[d, 0], ahead["ta"]),
        ]
        lax.fori_loop(0, 3, pack, 0)
        targets = (behind["gz"], ahead["gz"], behind["xy"], ahead["xy"])
        for kind, target in sorted(enumerate(targets), key=lambda entry: -entry[0]):
            copies.append(send(base_number + 2 + kind, ps.at[d, kind], pr.at[d, kind], target))

        before_local()

        def local(t, carry):
            psi = load_spinor(field, t)
            total = [[(jnp.zeros((8, 128), F32), jnp.zeros((8, 128), F32)) for _ in range(3)] for _ in range(4)]

            def up(v):
                return jnp.where(column_y == LY - 1, roll(v, LY - 1, 1) * sign[3], roll(v, -1, 1))

            def down(v):
                return jnp.where(column_y == 0, roll(v, 1 - LY, 1) * sign[3], roll(v, 1, 1))

            rebuild(total, link_times(ga, 3, t, map_half(project(psi, 3, True), up)), 3, True)
            rebuild(total, map_half(link_dagger(ga, 3, t, project(psi, 3, False)), down), 3, False)
            for ch in range(2):
                for i in range(6):
                    s, c = 2 * ch + i // 3, i % 3
                    re, im = psi[s][c][0] * MASS_TERM, psi[s][c][1] * MASS_TERM
                    for j in range(6):
                        vr, vi = psi[2 * ch + j // 3][j % 3]
                        mr, mi = cl[ch, 0, i * 6 + j, t], cl[ch, 1, i * 6 + j, t]
                        re = re + (mr * vr - mi * vi)
                        im = im + (mr * vi + mi * vr)
                    k = s * 3 + c
                    out[k, t] = base[k, t] - re + 0.5 * total[s][c][0]
                    out[12 + k, t] = base[12 + k, t] - im + 0.5 * total[s][c][1]
            return carry

        lax.fori_loop(0, T, local, 0)
        for copy in copies:
            copy.wait()

        def unpack(g, carry):
            for k in range(4):
                c = g * 4 + k
                z0, z1 = pr[d, 0, c] * last[1], pr[d, 1, c] * first[1]
                x0, x1 = pr[d, 2, c] * last[2], pr[d, 3, c] * first[2]
                new = []
                for t in range(T):
                    new.append((
                        jnp.where(row == 7, roll(z0, 7 - t, 0), roll(hb[0, t, c], -1, 0)),
                        jnp.where(row == 0, roll(z1, -t, 0), roll(hb[1, t, c], 1, 0)),
                        jnp.where(lane >= 128 - LY, roll(x0, 128 - LY - LY * t, 1), roll(hb[2, t, c], -LY, 1)),
                        jnp.where(lane < LY, roll(x1, -LY * t, 1), roll(hb[3, t, c], LY, 1)),
                    ))
                for t in range(T):
                    for kind in range(4):
                        hs[kind, t, c] = new[t][kind]
            return carry

        lax.fori_loop(0, 3, unpack, 0)

        def finish(t, carry):
            total = [[(jnp.zeros((8, 128), F32), jnp.zeros((8, 128), F32)) for _ in range(3)] for _ in range(4)]
            edge = jnp.where(t == T - 1, last[0], 1.0)
            rebuild(total, link_times(ga, 0, t, map_half(load_half(ht, d, t + 1), lambda v: v * edge)), 0, True)
            low = jnp.where(t == 0, first[0], 1.0)
            rebuild(total, map_half(load_half(gt, d, t), lambda v: v * low), 0, False)
            for mu in (1, 2):
                rebuild(total, link_times(ga, mu, t, load_half(hs, 2 * mu - 2, t)), mu, True)
                rebuild(total, load_half(hs, 2 * mu - 1, t), mu, False)
            for s in range(4):
                for c in range(3):
                    k = s * 3 + c
                    out[k, t] = out[k, t] + 0.5 * total[s][c][0]
                    out[12 + k, t] = out[12 + k, t] + 0.5 * total[s][c][1]
            return carry

        lax.fori_loop(0, T, finish, 0)

    mrows[...] = jnp.zeros(mrows.shape, F32)
    loads[0].wait()
    loads[1].wait()

    def rest():
        loads[2].wait()
        loads[3].wait()

    subtract_fine(0, itv, src, res, rest)

    top = row < BLK

    def to_columns(k, carry):
        for pair in range(2):
            parts = split_columns(res[k, 2 * pair], res[k, 2 * pair + 1], top)
            for col in range(2):
                rc[col, k, pl.ds(8 * pair, 8), :] = parts[col].astype(jnp.bfloat16).astype(F32)
        return carry

    lax.fori_loop(0, 24, to_columns, 0)
    loads[4].wait()
    group = 4
    for col in range(2):
        slot = slot_ref[col]

        def restrict(g, carry):
            re = [jnp.zeros((16, 128), F32) for _ in range(group)]
            im = [jnp.zeros((16, 128), F32) for _ in range(group)]
            for s in range(12):
                fr, fi = rc[col, s], rc[col, 12 + s]
                for j in range(group):
                    nr = nu[slot, 0, g * group + j, s].astype(F32)
                    ni = nu[slot, 1, g * group + j, s].astype(F32)
                    re[j] = re[j] + (nr * fr + ni * fi)
                    im[j] = im[j] + (nr * fi - ni * fr)
            for j in range(group):
                mrows[pl.ds((2 * col) * LANES + g * group + j, 1), :] = jnp.sum(re[j], axis=0, keepdims=True)
                mrows[pl.ds((2 * col + 1) * LANES + g * group + j, 1), :] = jnp.sum(im[j], axis=0, keepdims=True)
            return carry

        lax.fori_loop(0, 24 // group, restrict, 0)
    chooser = ((column_y // BLK) == row).astype(F32)
    value = lax.dot_general(
        chooser, mrows[...], (((1,), (1,)), ((), ())), precision=HIGHEST, preferred_element_type=F32
    )
    rhs[...] = value
    wbuf[0] = RELAX_WEIGHT * value
    loads[5].wait()

    nv = co.shape[-1]
    block = 8
    def pieces(vector, col):
        return [roll(vector, -LANES * (2 * col + ri), 1)[:, :nv] for ri in range(2)]

    def products(col, pairs, i, re, im):
        for k, (vr, vi) in pairs:
            yr, yi = co[k, 0, i, col], co[k, 1, i, col]
            a, b = yr * vr - yi * vi, yr * vi + yi * vr
            re, im = (a, b) if re is None else (re + a, im + b)
        return re, im

    for it in range(CITERS - 1):
        targets = [ahead["ta"], behind["ta"], ahead["gz"], behind["gz"], ahead["xy"], behind["xy"]]
        copies = [None] * 6
        for d in (4, 5, 0, 1, 2, 3):
            copies[d] = send(12 + it * 6 + d, wbuf.at[it], wr.at[it, d], targets[d ^ 1])
        own = wbuf[it]
        up, down = roll(own, -1, 0), roll(own, 1, 0)
        copies[2].wait()
        copies[3].wait()
        next_z, last_z = wr[it, 2], wr[it, 3]
        pairs = [
            [
                (0, pieces(own, col)),
                (7, pieces(up, col)),
                (8, pieces(down, col)),
                (3, pieces(own, 1) if col == 0 else pieces(next_z, 0)),
                (4, pieces(own, 0) if col == 1 else pieces(last_z, 1)),
            ]
            for col in range(2)
        ]

        def near(g, carry):
            for j in range(block):
                i = g * block + j
                for col in range(2):
                    re, im = products(col, pairs[col], i, None, None)
                    part[col, 0, i] = re
                    part[col, 1, i] = im
            return carry

        lax.fori_loop(0, nv // block, near, 0)
        for d in (0, 1, 4, 5):
            copies[d].wait()
        far_pairs = [
            [(k, pieces(wr[it, d], col)) for k, d in ((1, 0), (2, 1), (5, 4), (6, 5))] for col in range(2)
        ]

        def far(g, applied):
            for j in range(block):
                i = g * block + j
                for col in range(2):
                    sums = products(col, far_pairs[col], i, part[col, 0, i], part[col, 1, i])
                    for ri in range(2):
                        whole = jnp.sum(sums[ri], axis=1, keepdims=True)
                        applied = jnp.where(lane == LANES * (2 * col + ri) + i, whole, applied)
            return applied

        applied = lax.fori_loop(0, nv // block, far, jnp.zeros((8, 128), F32))
        w = wbuf[it]
        wbuf[it + 1] = w + RELAX_WEIGHT * (rhs[...] - (2.0 * w + applied))

    w = wbuf[CITERS - 1].astype(jnp.bfloat16).astype(F32)
    wexp[...] = lax.dot_general(
        w, chooser, (((0,), (0,)), ((), ())), precision=HIGHEST, preferred_element_type=F32
    )
    spins = 3
    step = 4
    for col in range(2):
        slot = slot_ref[col]

        def some_spins(q, carry):
            def over(g, totals):
                totals = list(totals)
                for j in range(step):
                    c = g * step + j
                    vr = wexp[pl.ds(2 * col * LANES + c, 1), :]
                    vi = wexp[pl.ds((2 * col + 1) * LANES + c, 1), :]
                    for m in range(spins):
                        nr = nu[slot, 0, c, q * spins + m].astype(F32)
                        ni = nu[slot, 1, c, q * spins + m].astype(F32)
                        totals[2 * m] = totals[2 * m] + (nr * vr - ni * vi)
                        totals[2 * m + 1] = totals[2 * m + 1] + (nr * vi + ni * vr)
                return tuple(totals)

            zero = jnp.zeros((16, 128), F32)
            totals = lax.fori_loop(0, nv // step, over, (zero,) * (2 * spins))
            for m in range(spins):
                rc[col, q * spins + m] = totals[2 * m]
                rc[col, 12 + q * spins + m] = totals[2 * m + 1]
            return carry

        lax.fori_loop(0, 12 // spins, some_spins, 0)

    def from_columns(k, carry):
        for pair in range(2):
            part_0 = rc[0, k, pl.ds(8 * pair, 8), :]
            part_1 = rc[1, k, pl.ds(8 * pair, 8), :]
            values = split_columns(part_0, part_1, top)
            for h in range(2):
                t = 2 * pair + h
                corr[k, t] = values[h]
                nit[k, t] = itv[k, t] + values[h]
        return carry

    lax.fori_loop(0, 24, from_columns, 0)
    store_it = pltpu.make_async_copy(nit, out_it, load_sem.at[6])
    store_it.start()
    subtract_fine(1, corr, res, res, lambda: None)
    store_res = pltpu.make_async_copy(res, out_res, load_sem.at[7])
    store_res.start()
    store_it.wait()
    store_res.wait()


def hand_over(it_in, res_in, it_out, res_out, it_mid, res_mid, sem):
    ways = [(it_in, it_mid, it_out), (res_in, res_mid, res_out)]
    inward = [pltpu.make_async_copy(a, b, sem.at[i]) for i, (a, b, _) in enumerate(ways)]
    outward = [pltpu.make_async_copy(b, c, sem.at[2 + i]) for i, (_, b, c) in enumerate(ways)]
    for copy in inward:
        copy.start()
    for first, second in zip(inward, outward):
        first.wait()
        second.start()
    for copy in outward:
        copy.wait()


def per_device(counts, source, iterate, gauge_links, clover, bc_sign, null_store, block_slot, coarse_links):
    lattice = source.shape[3:]
    T = lattice[0]
    spinor = (24,) + lattice
    columns = block_slot.size
    nv = null_store.shape[4]
    assert lattice == (BLK, 2 * BLK, BLK * LY) and columns == 2
    nulls = (columns,) + null_store.shape[3:6] + (BLK * BLK, BLK * LY)
    links = jnp.transpose(coarse_links, (0, 1, 2, 4, 5, 6, 7, 3))
    links = links.reshape(links.shape[:3] + (columns,) + links.shape[6:])
    gauge_shape = (4, 2, 9) + lattice
    clover_shape = (2, 2, 36) + lattice
    half = (12,) + lattice[1:]
    tile = lattice[1:]
    smem = pl.BlockSpec(memory_space=pltpu.SMEM)
    hbm = pl.BlockSpec(memory_space=pl.ANY)
    fine = jax.ShapeDtypeStruct(spinor, F32)
    n_copies = 12 + 6 * (CITERS - 1)
    outs = pl.pallas_call(
        functools.partial(kernel, counts),
        out_shape=(fine, fine),
        in_specs=[smem, smem] + [pl.BlockSpec(memory_space=pltpu.HBM)] * 6,
        out_specs=(hbm, hbm),
        scratch_shapes=[
            pltpu.VMEM(spinor, F32),
            pltpu.VMEM(spinor, F32),
            pltpu.VMEM(gauge_shape, F32),
            pltpu.VMEM(clover_shape, F32),
            pltpu.VMEM(nulls, jnp.bfloat16),
            pltpu.VMEM(links.shape, F32),
            pltpu.VMEM(spinor, F32),
            pltpu.VMEM(spinor, F32),
            pltpu.VMEM(spinor, F32),
            pltpu.VMEM((2, T + 1) + half, F32),
            pltpu.VMEM((2, T + 1) + half, F32),
            pltpu.VMEM((4, T) + half, F32),
            pltpu.VMEM((4, T) + half, F32),
            pltpu.VMEM((2, 4) + half, F32),
            pltpu.VMEM((2, 4) + half, F32),
            pltpu.VMEM((columns, 24, BLK * BLK, BLK * LY), F32),
            pltpu.VMEM((128, 128), F32),
            pltpu.VMEM((CITERS,) + tile, F32),
            pltpu.VMEM(tile, F32),
            pltpu.VMEM((CITERS - 1, 6) + tile, F32),
            pltpu.VMEM((columns, 2, nv, 8, nv), F32),
            pltpu.VMEM((128, 128), F32),
            pltpu.SemaphoreType.DMA((8,)),
            pltpu.SemaphoreType.DMA((n_copies,)),
            pltpu.SemaphoreType.DMA((n_copies,)),
        ],
        compiler_params=pltpu.CompilerParams(
            collective_id=0, has_side_effects=True, vmem_limit_bytes=67_043_328
        ),
    )(
        bc_sign,
        block_slot.reshape(-1),
        source.reshape(spinor),
        iterate.reshape(spinor),
        gauge_links.reshape(gauge_shape),
        clover.reshape(clover_shape),
        null_store.reshape(nulls),
        links,
    )
    outs = pl.pallas_call(
        hand_over,
        out_shape=(fine, fine),
        in_specs=[hbm, hbm],
        out_specs=(pl.BlockSpec(memory_space=pltpu.HBM),) * 2,
        scratch_shapes=[pltpu.VMEM(spinor, F32), pltpu.VMEM(spinor, F32), pltpu.SemaphoreType.DMA((4,))],
        compiler_params=pltpu.CompilerParams(vmem_limit_bytes=67_043_328),
    )(*outs)
    return tuple(out.reshape(source.shape) for out in outs)


def solution(mesh):
    placed = (
        P(None, None, None, "ta", "gz", "xy"),
        P(None, None, None, "ta", "gz", "xy"),
        P(None, None, None, None, "ta", "gz", "xy"),
        P(None, None, None, None, "ta", "gz", "xy"),
        P(),
        P("ta", "gz", "xy", None, None, None, None, None, None),
        P("ta", "gz", "xy"),
        P(None, None, None, None, "ta", "gz", "xy", None),
    )
    return jax.shard_map(
        functools.partial(per_device, dict(mesh.shape)),
        mesh=mesh,
        in_specs=placed,
        out_specs=(P(None, None, None, "ta", "gz", "xy"), P(None, None, None, "ta", "gz", "xy")),
        check_vma=False,
    )
```
